32 devices in a mesh: pa: 4 (over y, x), dev: 8 (over z, core).
Axes of the slice: x: 2, y: 2, z: 4, core: 2. Of those that a mesh axis runs over, the one named last changes fastest.
Arguments:
- wq_train: float32 [8, 4096, 1024], P('pa', 'dev'), may hold values from -6 to 6
- lock_learned_mats: float32 [8, 4096, 256], P('pa', 'dev'), may hold values from -6 to 6
- worth_learned_mats: float32 [8, 4096, 256], P('pa', 'dev'), may hold values from -6 to 6
- gain_train: float32 [8, 4096], P('pa', 'dev'), may hold values from 0.1 to 1.9
- train_slots: int32 [8], replicated, may hold values from 0 to 7, as said below
- serve_section: int32 [4], replicated, may hold values from 0 to 3, each once
- face_sequence: int32 [8, 2], replicated, may hold values from 0 to 1, each once within a row
Outputs:
- qkv_serve: bfloat16 [8, 8, 4096, 384], P('pa', 'dev')
The draws below stay inside these ranges and needn't reach their ends.
Inputs may be any that keep to these rules, and one draw needn't show every extreme that they name: `train_slots`: slot s lies on training section s // 2; every layer is held by exactly one slot, and layer l lies on section l % 4. A permutation: serving section q holds layers serve_section[q] * 2 to serve_section[q] * 2 + 2 - 1 in its slots, in order. `face_sequence`: each row is a permutation of the 2 head groups.
All inputs are finite; a program needn't handle non-finite values.
Results may differ from the reference program's by a relative error of at most 0.001.
Values may be sent and summed in bfloat16 or wider, within the bound.
A program may use at most 128 MiB of HBM per device.

```python
import jax
import jax.numpy as jnp
from jax import lax

BREADTH = 4096
FACE_SPAN = 128
GROUP = 4
HEADS_RANK = 1
LPS = 2
SECTIONS = 4
PEERS = 8
TIERS = 8
HQ = 8
LOCK_FACES = 2
LOCKS_PER_PEER = 1
CW = 384


def draw_train_slots(key, part):
    scores = jax.random.randint(key, (SECTIONS, LPS), 0, 1 << 20, dtype=jnp.int32) * LPS + jnp.arange(LPS, dtype=jnp.int32)[None, :]
    ranking = jnp.argsort(scores, axis=1, stable=True).astype(jnp.int32)
    layers = jnp.arange(SECTIONS, dtype=jnp.int32)[:, None] + ranking * SECTIONS
    return layers.reshape(TIERS)


def steps_of(rng, shape, shards, least, top_value):
    gain, own = 1.0, jax.random.fold_in(rng, 6)
    for axis_at, shards_of in shards:
        steps = jnp.exp(jax.random.uniform(jax.random.fold_in(own, axis_at), (shards_of,), jnp.float32, least / len(shards), top_value / len(shards)))
        gain = gain * jnp.repeat(steps, shape[axis_at] // shards_of).reshape([-1 if axis == axis_at else 1 for axis in range(len(shape))])
    return gain


def bell_draw(rng, shape, spread, limit, shards=(), held_as=jnp.bfloat16):
    gain = steps_of(rng, shape, shards, -0.22, 0.18) if shards else 1.0
    values = jax.random.normal(rng, shape, jnp.float32) * spread * gain
    return jnp.minimum(jnp.maximum(values, -limit), limit).astype(held_as)


def setup_inputs(seed: int = 0) -> dict:
    splits = jax.random.split(jax.random.key(seed), 8)
    return {
        "wq_train": bell_draw(splits[0], (TIERS, BREADTH, HQ * FACE_SPAN), 1.0, 6.0, ((0, 4), (1, 8)), jnp.float32),
        "lock_learned_mats": bell_draw(splits[1], (TIERS, BREADTH, LOCK_FACES * FACE_SPAN), 1.0, 6.0, ((0, 4), (1, 8)), jnp.float32),
        "worth_learned_mats": bell_draw(splits[2], (TIERS, BREADTH, LOCK_FACES * FACE_SPAN), 1.0, 6.0, ((0, 4), (1, 8)), jnp.float32),
        "gain_train": jnp.clip(1.0 + 0.18 * jax.random.normal(splits[3], (TIERS, BREADTH), jnp.float32), 0.1, 1.9),
        "train_slots": draw_train_slots(jax.random.fold_in(splits[7], 71), 0),
        "serve_section": jax.random.permutation(splits[5], SECTIONS).astype(jnp.int32),
        "face_sequence": jax.vmap(lambda own: jax.random.permutation(own, LOCK_FACES))(jax.random.split(splits[6], TIERS)).reshape((TIERS, LOCK_FACES)).astype(jnp.int32),
    }


def reference(wq_train, lock_learned_mats, worth_learned_mats, gain_train, train_slots, serve_section, face_sequence):
    slot_ids = jnp.arange(TIERS, dtype=jnp.int32)
    head_index = jnp.arange(HQ, dtype=jnp.int32)
    pair_number = (jnp.arange(PEERS, dtype=jnp.int32)[:, None] * LOCK_FACES) // PEERS + jnp.arange(LOCKS_PER_PEER, dtype=jnp.int32)[None, :]

    def one_slot(target):
        layer_id = (serve_section[target // LPS] * LPS + target % LPS).astype(jnp.int32)
        provider = jnp.sum(jnp.where(train_slots == layer_id, slot_ids, 0)).astype(jnp.int32)
        group_order = face_sequence[layer_id]
        q_source = group_order[head_index // GROUP] * GROUP + head_index % GROUP
        pair_provider = group_order[pair_number].reshape(-1)
        query_sel = wq_train[provider].reshape(BREADTH, HQ, FACE_SPAN)[:, q_source].reshape(BREADTH, PEERS, HEADS_RANK, FACE_SPAN)
        lock_picker = lock_learned_mats[provider].reshape(BREADTH, LOCK_FACES, FACE_SPAN)[:, pair_provider].reshape(BREADTH, PEERS, LOCKS_PER_PEER, FACE_SPAN)
        worth_picker = worth_learned_mats[provider].reshape(BREADTH, LOCK_FACES, FACE_SPAN)[:, pair_provider].reshape(BREADTH, PEERS, LOCKS_PER_PEER, FACE_SPAN)
        joined_cols = jnp.concatenate([query_sel, lock_picker, worth_picker], axis=2)
        joined_cols = joined_cols * gain_train[provider][:, None, None, None]
        return joined_cols.transpose(1, 0, 2, 3).reshape(PEERS, BREADTH, CW).astype(jnp.bfloat16)

    return lax.map(one_slot, jnp.arange(TIERS, dtype=jnp.int32))
```

```python
import functools
import itertools
import math

import jax
import jax.numpy as jnp
from jax import lax
from jax.experimental import pallas as pl
from jax.experimental.pallas import tpu as pltpu
from jax.sharding import PartitionSpec as P

FACE_SPAN = 128
GROUP = 4


def lookup(small_table, indices):
    entries = jnp.arange(small_table.shape[0], dtype=jnp.int32)
    return jnp.sum(jnp.where(indices[..., None] == entries, small_table, 0), axis=-1).astype(
        jnp.int32
    )


def local(
    wq_train,
    lock_learned_mats,
    worth_learned_mats,
    gain_train,
    train_slots,
    serve_section,
    face_sequence,
):
    per_section = wq_train.shape[0]
    row_count = wq_train.shape[1]
    query_width = wq_train.shape[2]
    key_width = lock_learned_mats.shape[2]
    query_heads = query_width // FACE_SPAN
    key_heads = key_width // FACE_SPAN
    sections = lax.axis_size("pa")
    rank_count = lax.axis_size("dev")
    my_section = lax.axis_index("pa")
    keys_each = max(key_heads // rank_count, 1)
    slot_ids = jnp.arange(train_slots.shape[0], dtype=jnp.int32)
    section_ids = jnp.arange(sections, dtype=jnp.int32)
    slot_index = jnp.arange(per_section, dtype=jnp.int32)
    folded = (
        jnp.concatenate([wq_train, lock_learned_mats, worth_learned_mats], axis=2)
        * gain_train[:, :, None]
    )
    folded = folded.astype(jnp.bfloat16)

    def source_slot(layers):
        return jnp.sum(jnp.where(train_slots == layers[..., None], slot_ids, 0), axis=-1).astype(
            jnp.int32
        )

    wanted_layers = lookup(serve_section, my_section) * per_section + slot_index
    held_layers = lookup(train_slots, my_section * per_section + slot_index)
    destination = jnp.sum(
        jnp.where(
            serve_section[None, :] == (held_layers // per_section)[:, None], section_ids[None, :], 0
        ),
        axis=-1,
    )
    send_pick = (destination[None, :] == section_ids[:, None]).astype(jnp.bfloat16)
    outgoing = jnp.einsum(
        "qj,jrc->qrc", send_pick, folded, preferred_element_type=jnp.float32
    ).astype(jnp.bfloat16)
    arrived = lax.all_to_all(outgoing, "pa", split_axis=0, concat_axis=0, tiled=True)
    anchor = source_slot(wanted_layers) // per_section
    recv_pick = (anchor[:, None] == section_ids[None, :]).astype(jnp.bfloat16)
    received = jnp.einsum(
        "jq,qrc->jrc", recv_pick, arrived, preferred_element_type=jnp.float32
    ).astype(jnp.bfloat16)
    head_index = jnp.arange(query_heads, dtype=jnp.int32)
    pair_number = (
        jnp.arange(rank_count, dtype=jnp.int32)[:, None] * key_heads // rank_count
        + jnp.arange(keys_each, dtype=jnp.int32)[None, :]
    )

    def arrange(layer_rows, layer_id):
        group_order = jnp.take(face_sequence, layer_id, axis=0)
        q_source = lookup(group_order, head_index // GROUP) * GROUP + head_index % GROUP
        pair_provider = lookup(group_order, pair_number).reshape(-1)
        query_part = layer_rows[:, :query_width].reshape(row_count, query_heads, FACE_SPAN)
        key_part = layer_rows[:, query_width : query_width + key_width].reshape(
            row_count, key_heads, FACE_SPAN
        )
        value_part = layer_rows[:, query_width + key_width :].reshape(
            row_count, key_heads, FACE_SPAN
        )
        query_sel = jnp.take(query_part, q_source, axis=1).reshape(
            row_count, rank_count, query_heads // rank_count, FACE_SPAN
        )
        lock_picker = jnp.take(key_part, pair_provider, axis=1).reshape(
            row_count, rank_count, keys_each, FACE_SPAN
        )
        worth_picker = jnp.take(value_part, pair_provider, axis=1).reshape(
            row_count, rank_count, keys_each, FACE_SPAN
        )
        joined_cols = jnp.concatenate([query_sel, lock_picker, worth_picker], axis=2)
        return joined_cols.transpose(1, 0, 2, 3).reshape(rank_count, row_count, -1)

    collected = []
    for slot in range(per_section):
        outgoing_cols = arrange(received[slot], wanted_layers[slot])
        collected.append(
            lax.all_to_all(outgoing_cols, "dev", split_axis=0, concat_axis=1, tiled=True)
        )
    result = jnp.stack(collected, axis=0)
    return result

MESH = pl.DeviceIdType.MESH
CORES = 2
MAX_ROUTES = 8


def routes_of(sections, per_section):
    groups = sections // per_section
    base = [g for g in range(groups) for _ in range(per_section)]
    seen = []
    for choice in itertools.product(range(groups), repeat=sections):
        if sorted(choice) == base:
            seen.append(choice)
    return seen


def section_route(table, section, ordinal, per_section):
    dest = 0
    for g in range(max(table) + 1):
        members = [q for q, own in enumerate(table) if own == g]
        dest = jnp.where(section // per_section == g, members[ordinal], dest)
    return dest


def fold_kernel(
    sizes, my_ref, slots_ref, serve_ref, face_ref, wq_ref, lock_ref, worth_ref, gain_ref, q_out, kv_out
):
    sections, per_section, query_heads, key_heads = sizes
    layer, _ = pick(sizes, pl.program_id(0), my_ref, slots_ref, serve_ref)
    gain = gain_ref[0]
    for h in range(query_heads):
        source = face_ref[layer, h // GROUP] * GROUP + h % GROUP
        cols = pl.ds(pl.multiple_of(source * FACE_SPAN, FACE_SPAN), FACE_SPAN)
        q_out[0, h] = (wq_ref[0, :, cols] * gain).astype(jnp.bfloat16)
    for g in range(key_heads):
        cols = pl.ds(pl.multiple_of(face_ref[layer, g] * FACE_SPAN, FACE_SPAN), FACE_SPAN)
        kv_out[0, g, :, :FACE_SPAN] = (lock_ref[0, :, cols] * gain).astype(jnp.bfloat16)
        kv_out[0, g, :, FACE_SPAN:] = (worth_ref[0, :, cols] * gain).astype(jnp.bfloat16)


def pick(sizes, ordinal, my_ref, slots_ref, serve_ref):
    sections, per_section, _, _ = sizes
    groups = sections // per_section
    mine = my_ref[0]
    block, count = jnp.int32(0), jnp.int32(0)
    for q in range(sections):
        own = serve_ref[q] % groups == mine // per_section
        block = jnp.where(own & (count == ordinal), serve_ref[q], block)
        count = count + own.astype(jnp.int32)
    layer = block * per_section + mine % per_section
    slot = jnp.int32(0)
    for i in range(per_section):
        slot = jnp.where(slots_ref[mine * per_section + i] == layer, i, slot)
    return layer, slot


def fold(wq, lock, worth, gain, my, slots, serve, face, sections):
    per_section, rows, query_width = wq.shape
    key_width = lock.shape[2]
    query_heads, key_heads = query_width // FACE_SPAN, key_width // FACE_SPAN
    sizes = (sections, per_section, query_heads, key_heads)
    tile = min(rows, 256)

    def source(o, i, my_ref, slots_ref, serve_ref, face_ref):
        return (pick(sizes, o, my_ref, slots_ref, serve_ref)[1], i, 0)

    def target(o, i, *_):
        return (o, 0, i, 0)

    return pl.pallas_call(
        functools.partial(fold_kernel, sizes),
        grid_spec=pltpu.PrefetchScalarGridSpec(
            num_scalar_prefetch=4,
            grid=(per_section, rows // tile),
            in_specs=[
                pl.BlockSpec((1, tile, query_width), source),
                pl.BlockSpec((1, tile, key_width), source),
                pl.BlockSpec((1, tile, key_width), source),
                pl.BlockSpec((1, tile, 1), source),
            ],
            out_specs=[
                pl.BlockSpec((1, query_heads, tile, FACE_SPAN), target),
                pl.BlockSpec((1, key_heads, tile, 2 * FACE_SPAN), target),
            ],
        ),
        out_shape=[
            jax.ShapeDtypeStruct((per_section, query_heads, rows, FACE_SPAN), jnp.bfloat16),
            jax.ShapeDtypeStruct((per_section, key_heads, rows, 2 * FACE_SPAN), jnp.bfloat16),
        ],
        name="fold",
    )(my, slots, serve, face, wq, lock, worth, gain[:, :, None])


def route_kernel(
    table, per_section, q_ref, kv_ref, out_ref, q_send, q_recv, kv_send, kv_recv, near_send, far_send
):
    sections = len(table)
    ranks = q_ref.shape[1]
    key_heads = kv_ref.shape[1]
    rows = q_ref.shape[2]
    chips = ranks // CORES
    span = chips // key_heads
    section = lax.axis_index("pa")
    rank = lax.axis_index("dev")
    chip, core = rank // CORES, rank % CORES
    slot = section % per_section

    barrier = pltpu.get_barrier_semaphore()

    def greet(i, carry):
        other = (section * ranks + rank + i) % (sections * ranks)
        pl.semaphore_signal(
            barrier, inc=1, device_id=(other // ranks, other % ranks), device_id_type=MESH
        )
        return carry

    lax.fori_loop(1, sections * ranks, greet, 0)
    pl.semaphore_wait(barrier, sections * ranks - 1)

    def q_place(j, d):
        return out_ref.at[j, 0, pl.ds(pl.multiple_of(d * rows, rows), rows), pl.ds(0, FACE_SPAN)]

    def kv_place(j, d):
        return out_ref.at[
            j, 0, pl.ds(pl.multiple_of(d * rows, rows), rows), pl.ds(FACE_SPAN, 2 * FACE_SPAN)
        ]

    def send(source, place, send_sem, recv_sem, to, wait=False):
        here = (to[0] == section) & (to[1] == rank)

        @pl.when(jnp.logical_not(here))
        def _():
            copy = pltpu.make_async_remote_copy(
                source, place, send_sem, recv_sem, device_id=to, device_id_type=MESH
            )
            copy.wait_send() if wait else copy.start()

        if not wait:

            @pl.when(here)
            def _():
                pltpu.make_async_copy(source, place, recv_sem).start()

    def send_kv(wait):
        for g in range(key_heads):
            for o in range(per_section):
                to = section_route(table, section, o, per_section)
                entry = jnp.clip(chip, g * span, g * span + span - 1)
                send(
                    kv_ref.at[o, g], kv_place(slot, rank), kv_send.at[o, g], kv_recv.at[slot, rank],
                    (to, entry * CORES + core), wait,
                )

    def send_q(wait):
        for step in range(ranks):
            for o in range(per_section):
                to = section_route(table, section, o, per_section)
                r = (rank + ranks // 2 + step) % ranks
                send(
                    q_ref.at[o, r], q_place(slot, rank), q_send.at[o, step], q_recv.at[slot, rank],
                    (to, r), wait,
                )

    def forward(wait):
        low = chip // span * span
        high = low + span - 1
        for near in range(chips):
            for j in range(per_section):
                c = (chip + near) % chips
                d = c * CORES + core
                place = kv_place(j, d)
                entry = jnp.clip(c, low, high)
                if not wait:
                    pltpu.make_async_copy(place, place, kv_recv.at[j, d]).wait()
                for up in (1, 0):
                    go = (
                        (chip >= entry) & (chip < high) if up else (chip <= entry) & (chip > low)
                    )

                    @pl.when(go)
                    def _():
                        copy = pltpu.make_async_remote_copy(
                            place, place, far_send.at[j, near, up], kv_recv.at[j, d],
                            device_id=(section, (chip + 2 * up - 1) * CORES + core),
                            device_id_type=MESH,
                        )
                        copy.wait_send() if wait else copy.start()

                copy = pltpu.make_async_remote_copy(
                    place, place, near_send.at[j, near], kv_recv.at[j, d],
                    device_id=(section, chip * CORES + 1 - core),
                    device_id_type=MESH,
                )
                copy.wait_send() if wait else copy.start()

    send_kv(False)
    send_q(False)
    forward(False)
    send_kv(True)
    send_q(True)
    forward(True)
    for j in range(per_section):
        for c in range(chips):
            d = c * CORES + 1 - core
            pltpu.make_async_copy(kv_place(j, d), kv_place(j, d), kv_recv.at[j, d]).wait()
        for d in range(ranks):
            pltpu.make_async_copy(q_place(j, d), q_place(j, d), q_recv.at[j, d]).wait()


def route(folded_q, folded_kv, table, number):
    per_section, ranks, rows, _ = folded_q.shape
    key_heads = folded_kv.shape[1]
    chips = ranks // CORES
    dma = pltpu.SemaphoreType.DMA
    return pl.pallas_call(
        functools.partial(route_kernel, table, per_section),
        out_shape=jax.ShapeDtypeStruct(
            (per_section, 1, ranks * rows, 3 * FACE_SPAN), jnp.bfloat16
        ),
        in_specs=[pl.BlockSpec(memory_space=pl.ANY)] * 2,
        out_specs=pl.BlockSpec(memory_space=pl.ANY),
        scratch_shapes=[
            dma((per_section, ranks)),
            dma((per_section, ranks)),
            dma((per_section, key_heads)),
            dma((per_section, ranks)),
            dma((per_section, chips)),
            dma((per_section, chips, 2)),
        ],
        compiler_params=pltpu.CompilerParams(collective_id=number, has_side_effects=True),
        name="route",
    )(folded_q, folded_kv)


def direct(
    wq_train, lock_learned_mats, worth_learned_mats, gain_train, train_slots, serve_section, face_sequence
):
    sections = lax.axis_size("pa")
    per_section = wq_train.shape[0]
    groups = sections // per_section
    my = lax.axis_index("pa").astype(jnp.int32).reshape(1)
    folded_q, folded_kv = fold(
        wq_train, lock_learned_mats, worth_learned_mats, gain_train,
        my, train_slots, serve_section, face_sequence, sections,
    )
    routes = routes_of(sections, per_section)
    known = jnp.array(routes, dtype=jnp.int32)
    matches = jnp.all(known == (serve_section % groups)[None, :], axis=1)
    chosen = jnp.sum(jnp.where(matches, jnp.arange(len(routes), dtype=jnp.int32), 0))
    return lax.switch(
        chosen,
        [functools.partial(route, table=t, number=i) for i, t in enumerate(routes)],
        folded_q,
        folded_kv,
    )


def fits(sections, per_section, ranks, query_heads, key_heads):
    if sections % per_section or ranks % (CORES * key_heads) or query_heads != ranks:
        return False
    ways, left = 1, sections
    while left:
        ways, left = ways * math.comb(left, per_section), left - per_section
    return ways <= MAX_ROUTES


def move(*arrays):
    wq_train, lock_learned_mats = arrays[:2]
    plain = fits(
        lax.axis_size("pa"),
        wq_train.shape[0],
        lax.axis_size("dev"),
        wq_train.shape[2] // FACE_SPAN,
        lock_learned_mats.shape[2] // FACE_SPAN,
    )
    return direct(*arrays) if plain else local(*arrays)


def solution(mesh):
    return jax.shard_map(
        move,
        mesh=mesh,
        in_specs=(
            P("pa", "dev", None),
            P("pa", "dev", None),
            P("pa", "dev", None),
            P("pa", "dev"),
            P(),
            P(),
            P(),
        ),
        out_specs=P("pa", "dev", None, None),
        check_vma=False,
    )
```

```python
import functools
import itertools
import math

import jax
import jax.numpy as jnp
from jax import lax
from jax.experimental import pallas as pl
from jax.experimental.pallas import tpu as pltpu
from jax.sharding import PartitionSpec as P

FACE_SPAN = 128
GROUP = 4


def lookup(small_table, indices):
    entries = jnp.arange(small_table.shape[0], dtype=jnp.int32)
    return jnp.sum(jnp.where(indices[..., None] == entries, small_table, 0), axis=-1).astype(
        jnp.int32
    )


def local(
    wq_train,
    lock_learned_mats,
    worth_learned_mats,
    gain_train,
    train_slots,
    serve_section,
    face_sequence,
):
    per_section = wq_train.shape[0]
    row_count = wq_train.shape[1]
    query_width = wq_train.shape[2]
    key_width = lock_learned_mats.shape[2]
    query_heads = query_width // FACE_SPAN
    key_heads = key_width // FACE_SPAN
    sections = lax.axis_size("pa")
    rank_count = lax.axis_size("dev")
    my_section = lax.axis_index("pa")
    keys_each = max(key_heads // rank_count, 1)
    slot_ids = jnp.arange(train_slots.shape[0], dtype=jnp.int32)
    section_ids = jnp.arange(sections, dtype=jnp.int32)
    slot_index = jnp.arange(per_section, dtype=jnp.int32)
    folded = (
        jnp.concatenate([wq_train, lock_learned_mats, worth_learned_mats], axis=2)
        * gain_train[:, :, None]
    )
    folded = folded.astype(jnp.bfloat16)

    def source_slot(layers):
        return jnp.sum(jnp.where(train_slots == layers[..., None], slot_ids, 0), axis=-1).astype(
            jnp.int32
        )

    wanted_layers = lookup(serve_section, my_section) * per_section + slot_index
    held_layers = lookup(train_slots, my_section * per_section + slot_index)
    destination = jnp.sum(
        jnp.where(
            serve_section[None, :] == (held_layers // per_section)[:, None], section_ids[None, :], 0
        ),
        axis=-1,
    )
    send_pick = (destination[None, :] == section_ids[:, None]).astype(jnp.bfloat16)
    outgoing = jnp.einsum(
        "qj,jrc->qrc", send_pick, folded, preferred_element_type=jnp.float32
    ).astype(jnp.bfloat16)
    arrived = lax.all_to_all(outgoing, "pa", split_axis=0, concat_axis=0, tiled=True)
    anchor = source_slot(wanted_layers) // per_section
    recv_pick = (anchor[:, None] == section_ids[None, :]).astype(jnp.bfloat16)
    received = jnp.einsum(
        "jq,qrc->jrc", recv_pick, arrived, preferred_element_type=jnp.float32
    ).astype(jnp.bfloat16)
    head_index = jnp.arange(query_heads, dtype=jnp.int32)
    pair_number = (
        jnp.arange(rank_count, dtype=jnp.int32)[:, None] * key_heads // rank_count
        + jnp.arange(keys_each, dtype=jnp.int32)[None, :]
    )

    def arrange(layer_rows, layer_id):
        group_order = jnp.take(face_sequence, layer_id, axis=0)
        q_source = lookup(group_order, head_index // GROUP) * GROUP + head_index % GROUP
        pair_provider = lookup(group_order, pair_number).reshape(-1)
        query_part = layer_rows[:, :query_width].reshape(row_count, query_heads, FACE_SPAN)
        key_part = layer_rows[:, query_width : query_width + key_width].reshape(
            row_count, key_heads, FACE_SPAN
        )
        value_part = layer_rows[:, query_width + key_width :].reshape(
            row_count, key_heads, FACE_SPAN
        )
        query_sel = jnp.take(query_part, q_source, axis=1).reshape(
            row_count, rank_count, query_heads // rank_count, FACE_SPAN
        )
        lock_picker = jnp.take(key_part, pair_provider, axis=1).reshape(
            row_count, rank_count, keys_each, FACE_SPAN
        )
        worth_picker = jnp.take(value_part, pair_provider, axis=1).reshape(
            row_count, rank_count, keys_each, FACE_SPAN
        )
        joined_cols = jnp.concatenate([query_sel, lock_picker, worth_picker], axis=2)
        return joined_cols.transpose(1, 0, 2, 3).reshape(rank_count, row_count, -1)

    collected = []
    for slot in range(per_section):
        outgoing_cols = arrange(received[slot], wanted_layers[slot])
        collected.append(
            lax.all_to_all(outgoing_cols, "dev", split_axis=0, concat_axis=1, tiled=True)
        )
    result = jnp.stack(collected, axis=0)
    return result

MESH = pl.DeviceIdType.MESH
CORES = 2
MAX_ROUTES = 8
PARTS = 4


def routes_of(sections, per_section):
    groups = sections // per_section
    base = [g for g in range(groups) for _ in range(per_section)]
    seen = []
    for choice in itertools.product(range(groups), repeat=sections):
        if sorted(choice) == base:
            seen.append(choice)
    return seen


def section_route(table, section, ordinal, per_section):
    dest = 0
    for g in range(max(table) + 1):
        members = [q for q, own in enumerate(table) if own == g]
        dest = jnp.where(section // per_section == g, members[ordinal], dest)
    return dest


def fold_kernel(
    sizes, my_ref, slots_ref, serve_ref, face_ref, wq_ref, lock_ref, worth_ref, gain_ref, q_out, kv_out
):
    sections, per_section, query_heads, key_heads = sizes
    layer, _ = pick(sizes, pl.program_id(0), my_ref, slots_ref, serve_ref)
    gain = gain_ref[0]
    for h in range(query_heads):
        source = face_ref[layer, h // GROUP] * GROUP + h % GROUP
        cols = pl.ds(pl.multiple_of(source * FACE_SPAN, FACE_SPAN), FACE_SPAN)
        q_out[0, h] = (wq_ref[0, :, cols] * gain).astype(jnp.bfloat16)
    for g in range(key_heads):
        cols = pl.ds(pl.multiple_of(face_ref[layer, g] * FACE_SPAN, FACE_SPAN), FACE_SPAN)
        kv_out[0, g, :, :FACE_SPAN] = (lock_ref[0, :, cols] * gain).astype(jnp.bfloat16)
        kv_out[0, g, :, FACE_SPAN:] = (worth_ref[0, :, cols] * gain).astype(jnp.bfloat16)


def pick(sizes, ordinal, my_ref, slots_ref, serve_ref):
    sections, per_section, _, _ = sizes
    groups = sections // per_section
    mine = my_ref[0]
    block, count = jnp.int32(0), jnp.int32(0)
    for q in range(sections):
        own = serve_ref[q] % groups == mine // per_section
        block = jnp.where(own & (count == ordinal), serve_ref[q], block)
        count = count + own.astype(jnp.int32)
    layer = block * per_section + mine % per_section
    slot = jnp.int32(0)
    for i in range(per_section):
        slot = jnp.where(slots_ref[mine * per_section + i] == layer, i, slot)
    return layer, slot


def fold(wq, lock, worth, gain, my, slots, serve, face, sections):
    per_section, rows, query_width = wq.shape
    key_width = lock.shape[2]
    query_heads, key_heads = query_width // FACE_SPAN, key_width // FACE_SPAN
    sizes = (sections, per_section, query_heads, key_heads)
    tile = min(rows, 256)

    def source(o, i, my_ref, slots_ref, serve_ref, face_ref):
        return (pick(sizes, o, my_ref, slots_ref, serve_ref)[1], i, 0)

    def target(o, i, *_):
        return (o, 0, i, 0)

    return pl.pallas_call(
        functools.partial(fold_kernel, sizes),
        grid_spec=pltpu.PrefetchScalarGridSpec(
            num_scalar_prefetch=4,
            grid=(per_section, rows // tile),
            in_specs=[
                pl.BlockSpec((1, tile, query_width), source),
                pl.BlockSpec((1, tile, key_width), source),
                pl.BlockSpec((1, tile, key_width), source),
                pl.BlockSpec((1, tile, 1), source),
            ],
            out_specs=[
                pl.BlockSpec((1, query_heads, tile, FACE_SPAN), target),
                pl.BlockSpec((1, key_heads, tile, 2 * FACE_SPAN), target),
            ],
        ),
        out_shape=[
            jax.ShapeDtypeStruct((per_section, query_heads, rows, FACE_SPAN), jnp.bfloat16),
            jax.ShapeDtypeStruct((per_section, key_heads, rows, 2 * FACE_SPAN), jnp.bfloat16),
        ],
        name="fold",
    )(my, slots, serve, face, wq, lock, worth, gain[:, :, None])


def route_kernel(
    table, per_section, q_ref, kv_ref, out_ref, q_send, q_recv, kv_send, kv_recv, near_send, far_send, kv_held, kept
):
    sections = len(table)
    ranks = q_ref.shape[1]
    key_heads = kv_ref.shape[1]
    rows = q_ref.shape[2]
    chips = ranks // CORES
    span = chips // key_heads
    section = lax.axis_index("pa")
    rank = lax.axis_index("dev")
    chip, core = rank // CORES, rank % CORES
    slot = section % per_section

    barrier = pltpu.get_barrier_semaphore()

    def greet(i, carry):
        other = (section * ranks + rank + i) % (sections * ranks)
        pl.semaphore_signal(
            barrier, inc=1, device_id=(other // ranks, other % ranks), device_id_type=MESH
        )
        return carry

    lax.fori_loop(1, sections * ranks, greet, 0)
    pl.semaphore_wait(barrier, sections * ranks - 1)

    def q_place(j, d):
        return out_ref.at[j, 0, pl.ds(pl.multiple_of(d * rows, rows), rows), pl.ds(0, FACE_SPAN)]

    part = rows // PARTS

    def kv_place(j, d, h):
        return kv_held.at[j, d, pl.ds(h * part, part)]

    def keep(j, d, h, index):
        first = pl.multiple_of(d * rows + h * part, part)
        place = out_ref.at[j, 0, pl.ds(first, part), pl.ds(FACE_SPAN, 2 * FACE_SPAN)]
        return pltpu.make_async_copy(kv_place(j, d, h), place, kept.at[j, index, h])

    def send(source, place, send_sem, recv_sem, to, wait=False):
        here = (to[0] == section) & (to[1] == rank)

        @pl.when(jnp.logical_not(here))
        def _():
            copy = pltpu.make_async_remote_copy(
                source, place, send_sem, recv_sem, device_id=to, device_id_type=MESH
            )
            copy.wait_send() if wait else copy.start()

        if not wait:

            @pl.when(here)
            def _():
                pltpu.make_async_copy(source, place, recv_sem).start()

    def send_kv(wait):
        for h, g, o in itertools.product(range(PARTS), range(key_heads), range(per_section)):
            to = section_route(table, section, o, per_section)
            entry = jnp.clip(chip, g * span, g * span + span - 1)
            send(
                kv_ref.at[o, g, pl.ds(h * part, part)], kv_place(slot, rank, h),
                kv_send.at[o, g, h], kv_recv.at[slot, rank, h],
                (to, entry * CORES + core), wait,
            )

    def send_q(wait):
        for step in range(ranks):
            for o in range(per_section):
                to = section_route(table, section, o, per_section)
                r = (rank + ranks // 2 + step) % ranks
                send(
                    q_ref.at[o, r], q_place(slot, rank), q_send.at[o, step], q_recv.at[slot, rank],
                    (to, r), wait,
                )

    def forward(wait):
        low = chip // span * span
        high = low + span - 1
        turn = jnp.where(chip < chips // 2, 1, chips - 1)
        for near in range(chips):
            for h, j in itertools.product(range(PARTS), range(per_section)):
                c = (chip + turn * near) % chips
                d = c * CORES + core
                place = kv_place(j, d, h)
                entry = jnp.clip(c, low, high)
                if not wait:
                    pltpu.make_async_copy(place, place, kv_recv.at[j, d, h]).wait()
                for up in (1, 0):
                    go = (
                        (chip >= entry) & (chip < high) if up else (chip <= entry) & (chip > low)
                    )

                    @pl.when(go)
                    def _():
                        copy = pltpu.make_async_remote_copy(
                            place, place, far_send.at[j, near, h, up], kv_recv.at[j, d, h],
                            device_id=(section, (chip + 2 * up - 1) * CORES + core),
                            device_id_type=MESH,
                        )
                        copy.wait_send() if wait else copy.start()

                copy = pltpu.make_async_remote_copy(
                    place, place, near_send.at[j, near, h], kv_recv.at[j, d, h],
                    device_id=(section, chip * CORES + 1 - core),
                    device_id_type=MESH,
                )
                copy.wait_send() if wait else copy.start()
                copy = keep(j, d, h, near)
                copy.wait() if wait else copy.start()

    send_kv(False)
    send_q(False)
    forward(False)
    for c, h, j in itertools.product(range(chips), range(PARTS), range(per_section)):
        d = c * CORES + 1 - core
        place = kv_place(j, d, h)
        pltpu.make_async_copy(place, place, kv_recv.at[j, d, h]).wait()
        keep(j, d, h, chips + c).start()
    send_kv(True)
    send_q(True)
    forward(True)
    for c, h, j in itertools.product(range(chips), range(PARTS), range(per_section)):
        keep(j, c * CORES + 1 - core, h, chips + c).wait()
    for j in range(per_section):
        for d in range(ranks):
            pltpu.make_async_copy(q_place(j, d), q_place(j, d), q_recv.at[j, d]).wait()


def route(folded_q, folded_kv, table, number):
    per_section, ranks, rows, _ = folded_q.shape
    key_heads = folded_kv.shape[1]
    chips = ranks // CORES
    dma = pltpu.SemaphoreType.DMA
    return pl.pallas_call(
        functools.partial(route_kernel, table, per_section),
        out_shape=jax.ShapeDtypeStruct(
            (per_section, 1, ranks * rows, 3 * FACE_SPAN), jnp.bfloat16
        ),
        in_specs=[pl.BlockSpec(memory_space=pl.ANY)] * 2,
        out_specs=pl.BlockSpec(memory_space=pl.ANY),
        scratch_shapes=[
            dma((per_section, ranks)),
            dma((per_section, ranks)),
            dma((per_section, key_heads, PARTS)),
            dma((per_section, ranks, PARTS)),
            dma((per_section, chips, PARTS)),
            dma((per_section, chips, PARTS, 2)),
            pltpu.VMEM((per_section, ranks, rows, 2 * FACE_SPAN), jnp.bfloat16),
            dma((per_section, ranks, PARTS)),
        ],
        compiler_params=pltpu.CompilerParams(collective_id=number, has_side_effects=True),
        name="route",
    )(folded_q, folded_kv)


def direct(
    wq_train, lock_learned_mats, worth_learned_mats, gain_train, train_slots, serve_section, face_sequence
):
    sections = lax.axis_size("pa")
    per_section = wq_train.shape[0]
    groups = sections // per_section
    my = lax.axis_index("pa").astype(jnp.int32).reshape(1)
    folded_q, folded_kv = fold(
        wq_train, lock_learned_mats, worth_learned_mats, gain_train,
        my, train_slots, serve_section, face_sequence, sections,
    )
    routes = routes_of(sections, per_section)
    known = jnp.array(routes, dtype=jnp.int32)
    matches = jnp.all(known == (serve_section % groups)[None, :], axis=1)
    chosen = jnp.sum(jnp.where(matches, jnp.arange(len(routes), dtype=jnp.int32), 0))
    return lax.switch(
        chosen,
        [functools.partial(route, table=t, number=i) for i, t in enumerate(routes)],
        folded_q,
        folded_kv,
    )


def fits(sections, per_section, ranks, query_heads, key_heads):
    if sections % per_section or ranks % (CORES * key_heads) or query_heads != ranks:
        return False
    ways, left = 1, sections
    while left:
        ways, left = ways * math.comb(left, per_section), left - per_section
    return ways <= MAX_ROUTES


def move(*arrays):
    wq_train, lock_learned_mats = arrays[:2]
    plain = fits(
        lax.axis_size("pa"),
        wq_train.shape[0],
        lax.axis_size("dev"),
        wq_train.shape[2] // FACE_SPAN,
        lock_learned_mats.shape[2] // FACE_SPAN,
    )
    return direct(*arrays) if plain else local(*arrays)


def solution(mesh):
    return jax.shard_map(
        move,
        mesh=mesh,
        in_specs=(
            P("pa", "dev", None),
            P("pa", "dev", None),
            P("pa", "dev", None),
            P("pa", "dev"),
            P(),
            P(),
            P(),
        ),
        out_specs=P("pa", "dev", None, None),
        check_vma=False,
    )
```

```python
import functools
import itertools
import math

import jax
import jax.numpy as jnp
from jax import lax
from jax.experimental import pallas as pl
from jax.experimental.pallas import tpu as pltpu
from jax.sharding import PartitionSpec as P

FACE_SPAN = 128
GROUP = 4


def lookup(small_table, indices):
    entries = jnp.arange(small_table.shape[0], dtype=jnp.int32)
    return jnp.sum(jnp.where(indices[..., None] == entries, small_table, 0), axis=-1).astype(
        jnp.int32
    )


def local(
    wq_train,
    lock_learned_mats,
    worth_learned_mats,
    gain_train,
    train_slots,
    serve_section,
    face_sequence,
):
    per_section = wq_train.shape[0]
    row_count = wq_train.shape[1]
    query_width = wq_train.shape[2]
    key_width = lock_learned_mats.shape[2]
    query_heads = query_width // FACE_SPAN
    key_heads = key_width // FACE_SPAN
    sections = lax.axis_size("pa")
    rank_count = lax.axis_size("dev")
    my_section = lax.axis_index("pa")
    keys_each = max(key_heads // rank_count, 1)
    slot_ids = jnp.arange(train_slots.shape[0], dtype=jnp.int32)
    section_ids = jnp.arange(sections, dtype=jnp.int32)
    slot_index = jnp.arange(per_section, dtype=jnp.int32)
    folded = (
        jnp.concatenate([wq_train, lock_learned_mats, worth_learned_mats], axis=2)
        * gain_train[:, :, None]
    )
    folded = folded.astype(jnp.bfloat16)

    def source_slot(layers):
        return jnp.sum(jnp.where(train_slots == layers[..., None], slot_ids, 0), axis=-1).astype(
            jnp.int32
        )

    wanted_layers = lookup(serve_section, my_section) * per_section + slot_index
    held_layers = lookup(train_slots, my_section * per_section + slot_index)
    destination = jnp.sum(
        jnp.where(
            serve_section[None, :] == (held_layers // per_section)[:, None], section_ids[None, :], 0
        ),
        axis=-1,
    )
    send_pick = (destination[None, :] == section_ids[:, None]).astype(jnp.bfloat16)
    outgoing = jnp.einsum(
        "qj,jrc->qrc", send_pick, folded, preferred_element_type=jnp.float32
    ).astype(jnp.bfloat16)
    arrived = lax.all_to_all(outgoing, "pa", split_axis=0, concat_axis=0, tiled=True)
    anchor = source_slot(wanted_layers) // per_section
    recv_pick = (anchor[:, None] == section_ids[None, :]).astype(jnp.bfloat16)
    received = jnp.einsum(
        "jq,qrc->jrc", recv_pick, arrived, preferred_element_type=jnp.float32
    ).astype(jnp.bfloat16)
    head_index = jnp.arange(query_heads, dtype=jnp.int32)
    pair_number = (
        jnp.arange(rank_count, dtype=jnp.int32)[:, None] * key_heads // rank_count
        + jnp.arange(keys_each, dtype=jnp.int32)[None, :]
    )

    def arrange(layer_rows, layer_id):
        group_order = jnp.take(face_sequence, layer_id, axis=0)
        q_source = lookup(group_order, head_index // GROUP) * GROUP + head_index % GROUP
        pair_provider = lookup(group_order, pair_number).reshape(-1)
        query_part = layer_rows[:, :query_width].reshape(row_count, query_heads, FACE_SPAN)
        key_part = layer_rows[:, query_width : query_width + key_width].reshape(
            row_count, key_heads, FACE_SPAN
        )
        value_part = layer_rows[:, query_width + key_width :].reshape(
            row_count, key_heads, FACE_SPAN
        )
        query_sel = jnp.take(query_part, q_source, axis=1).reshape(
            row_count, rank_count, query_heads // rank_count, FACE_SPAN
        )
        lock_picker = jnp.take(key_part, pair_provider, axis=1).reshape(
            row_count, rank_count, keys_each, FACE_SPAN
        )
        worth_picker = jnp.take(value_part, pair_provider, axis=1).reshape(
            row_count, rank_count, keys_each, FACE_SPAN
        )
        joined_cols = jnp.concatenate([query_sel, lock_picker, worth_picker], axis=2)
        return joined_cols.transpose(1, 0, 2, 3).reshape(rank_count, row_count, -1)

    collected = []
    for slot in range(per_section):
        outgoing_cols = arrange(received[slot], wanted_layers[slot])
        collected.append(
            lax.all_to_all(outgoing_cols, "dev", split_axis=0, concat_axis=1, tiled=True)
        )
    result = jnp.stack(collected, axis=0)
    return result

MESH = pl.DeviceIdType.MESH
CORES = 2
MAX_ROUTES = 8
PARTS = 4


def routes_of(sections, per_section):
    groups = sections // per_section
    base = [g for g in range(groups) for _ in range(per_section)]
    seen = []
    for choice in itertools.product(range(groups), repeat=sections):
        if sorted(choice) == base:
            seen.append(choice)
    return seen


def section_route(table, section, ordinal, per_section):
    dest = 0
    for g in range(max(table) + 1):
        members = [q for q, own in enumerate(table) if own == g]
        dest = jnp.where(section // per_section == g, members[ordinal], dest)
    return dest


def fold_kernel(
    sizes, my_ref, slots_ref, serve_ref, face_ref, wq_ref, lock_ref, worth_ref, gain_ref, q_out, kv_out
):
    sections, per_section, query_heads, key_heads = sizes
    layer, slot = pick(sizes, pl.program_id(0), my_ref, slots_ref, serve_ref)
    row = gain_ref[0:1]
    for i in range(1, per_section):
        row = jnp.where(slot == i, gain_ref[i : i + 1], row)
    gain = jnp.broadcast_to(row, (FACE_SPAN, row.shape[1])).T
    for h in range(query_heads):
        source = face_ref[layer, h // GROUP] * GROUP + h % GROUP
        cols = pl.ds(pl.multiple_of(source * FACE_SPAN, FACE_SPAN), FACE_SPAN)
        q_out[0, h] = (wq_ref[0, :, cols] * gain).astype(jnp.bfloat16)
    for g in range(key_heads):
        cols = pl.ds(pl.multiple_of(face_ref[layer, g] * FACE_SPAN, FACE_SPAN), FACE_SPAN)
        kv_out[0, g, :, :FACE_SPAN] = (lock_ref[0, :, cols] * gain).astype(jnp.bfloat16)
        kv_out[0, g, :, FACE_SPAN:] = (worth_ref[0, :, cols] * gain).astype(jnp.bfloat16)


def pick(sizes, ordinal, my_ref, slots_ref, serve_ref):
    sections, per_section, _, _ = sizes
    groups = sections // per_section
    mine = my_ref[0]
    block, count = jnp.int32(0), jnp.int32(0)
    for q in range(sections):
        own = serve_ref[q] % groups == mine // per_section
        block = jnp.where(own & (count == ordinal), serve_ref[q], block)
        count = count + own.astype(jnp.int32)
    layer = block * per_section + mine % per_section
    slot = jnp.int32(0)
    for i in range(per_section):
        slot = jnp.where(slots_ref[mine * per_section + i] == layer, i, slot)
    return layer, slot


def fold(wq, lock, worth, gain, my, slots, serve, face, sections):
    per_section, rows, query_width = wq.shape
    key_width = lock.shape[2]
    query_heads, key_heads = query_width // FACE_SPAN, key_width // FACE_SPAN
    sizes = (sections, per_section, query_heads, key_heads)
    tile = min(rows, 256)

    def source(o, i, my_ref, slots_ref, serve_ref, face_ref):
        return (pick(sizes, o, my_ref, slots_ref, serve_ref)[1], i, 0)

    def target(o, i, *_):
        return (o, 0, i, 0)

    return pl.pallas_call(
        functools.partial(fold_kernel, sizes),
        grid_spec=pltpu.PrefetchScalarGridSpec(
            num_scalar_prefetch=4,
            grid=(per_section, rows // tile),
            in_specs=[
                pl.BlockSpec((1, tile, query_width), source),
                pl.BlockSpec((1, tile, key_width), source),
                pl.BlockSpec((1, tile, key_width), source),
                pl.BlockSpec((per_section, tile), lambda o, i, *_: (0, i)),
            ],
            out_specs=[
                pl.BlockSpec((1, query_heads, tile, FACE_SPAN), target),
                pl.BlockSpec((1, key_heads, tile, 2 * FACE_SPAN), target),
            ],
        ),
        out_shape=[
            jax.ShapeDtypeStruct((per_section, query_heads, rows, FACE_SPAN), jnp.bfloat16),
            jax.ShapeDtypeStruct((per_section, key_heads, rows, 2 * FACE_SPAN), jnp.bfloat16),
        ],
        name="fold",
    )(my, slots, serve, face, wq, lock, worth, gain)


def route_kernel(
    table, per_section, q_ref, kv_ref, out_ref, q_send, q_recv, kv_send, kv_recv, near_send, far_send, kv_held, kept,
    passing, pass_send, pass_recv
):
    sections = len(table)
    ranks = q_ref.shape[1]
    key_heads = kv_ref.shape[1]
    rows = q_ref.shape[2]
    chips = ranks // CORES
    span = chips // key_heads
    section = lax.axis_index("pa")
    rank = lax.axis_index("dev")
    chip, core = rank // CORES, rank % CORES
    slot = section % per_section
    stay = all(own == q // per_section for q, own in enumerate(table))

    barrier = pltpu.get_barrier_semaphore()

    def greet(i, carry):
        other = (section * ranks + rank + i) % (sections * ranks)
        pl.semaphore_signal(
            barrier, inc=1, device_id=(other // ranks, other % ranks), device_id_type=MESH
        )
        return carry

    lax.fori_loop(1, sections * ranks, greet, 0)
    pl.semaphore_wait(barrier, sections * ranks - 1)

    def q_place(j, d):
        return out_ref.at[j, 0, pl.ds(pl.multiple_of(d * rows, rows), rows), pl.ds(0, FACE_SPAN)]

    part = rows // PARTS

    def kv_place(j, d, h):
        return kv_held.at[j, d, pl.ds(h * part, part)]

    def keep(j, d, h, index):
        first = pl.multiple_of(d * rows + h * part, part)
        place = out_ref.at[j, 0, pl.ds(first, part), pl.ds(FACE_SPAN, 2 * FACE_SPAN)]
        return pltpu.make_async_copy(kv_place(j, d, h), place, kept.at[j, index, h])

    def send(source, place, send_sem, recv_sem, to, wait=False):
        here = (to[0] == section) & (to[1] == rank)

        @pl.when(jnp.logical_not(here))
        def _():
            copy = pltpu.make_async_remote_copy(
                source, place, send_sem, recv_sem, device_id=to, device_id_type=MESH
            )
            copy.wait_send() if wait else copy.start()

        if not wait:

            @pl.when(here)
            def _():
                pltpu.make_async_copy(source, place, recv_sem).start()

    def send_kv(wait):
        for h, g, o in itertools.product(range(PARTS), range(key_heads), range(per_section)):
            to = section_route(table, section, o, per_section)
            source = kv_ref.at[o, g, pl.ds(h * part, part)]
            sent = kv_send.at[o, g, h]
            if stay:
                entry = jnp.clip(chip, g * span, g * span + span - 1)
                send(
                    source, kv_place(slot, rank, h), sent, kv_recv.at[slot, rank, h],
                    (to, entry * CORES + core), wait,
                )
                continue

            @pl.when(chip // span == g)
            def _():
                send(
                    source, kv_place(slot, rank, h), sent, kv_recv.at[slot, rank, h],
                    (to, rank), wait,
                )

            @pl.when(chip // span != g)
            def _():
                send(
                    source, pass_place(slot, g, h), sent, pass_recv.at[slot, g, h],
                    (to, rank), wait,
                )

    def pass_place(j, g, h):
        return passing.at[j, g, pl.ds(h * part, part)]

    def relay(h, wait):
        for g, j in itertools.product(range(key_heads), range(per_section)):

            @pl.when(chip // span != g)
            def _():
                place = pass_place(j, g, h)
                entry = jnp.clip(chip, g * span, g * span + span - 1)
                if not wait:
                    pltpu.make_async_copy(place, place, pass_recv.at[j, g, h]).wait()
                copy = pltpu.make_async_remote_copy(
                    place, kv_place(j, rank, h), pass_send.at[j, g, h], kv_recv.at[j, rank, h],
                    device_id=(section, entry * CORES + core),
                    device_id_type=MESH,
                )
                copy.wait_send() if wait else copy.start()

    def send_q(steps, wait):
        for step in steps:
            for o in range(per_section):
                to = section_route(table, section, o, per_section)
                r = (rank + ranks // 2 + step) % ranks
                send(
                    q_ref.at[o, r], q_place(slot, rank), q_send.at[o, step], q_recv.at[slot, rank],
                    (to, r), wait,
                )

    def forward(near, h, wait):
        low = chip // span * span
        high = low + span - 1
        turn = jnp.where(chip < chips // 2, 1, chips - 1)
        for j in range(per_section):
            c = (chip + turn * near) % chips
            d = c * CORES + core
            place = kv_place(j, d, h)
            entry = jnp.clip(c, low, high)
            if not wait:
                pltpu.make_async_copy(place, place, kv_recv.at[j, d, h]).wait()
            for up in (1, 0):
                go = (
                    (chip >= entry) & (chip < high) if up else (chip <= entry) & (chip > low)
                )

                @pl.when(go)
                def _():
                    copy = pltpu.make_async_remote_copy(
                        place, place, far_send.at[j, near, h, up], kv_recv.at[j, d, h],
                        device_id=(section, (chip + 2 * up - 1) * CORES + core),
                        device_id_type=MESH,
                    )
                    copy.wait_send() if wait else copy.start()

            copy = pltpu.make_async_remote_copy(
                place, place, near_send.at[j, near, h], kv_recv.at[j, d, h],
                device_id=(section, chip * CORES + 1 - core),
                device_id_type=MESH,
            )
            copy.wait_send() if wait else copy.start()
            copy = keep(j, d, h, near)
            copy.wait() if wait else copy.start()

    send_kv(False)
    if stay:
        send_q(range(ranks), False)
    for h in range(PARTS):
        if not stay:
            send_q(range(ranks * h // PARTS, ranks * (h + 1) // PARTS), False)
            relay(h, False)
        forward(0, h, False)
    for near, h in itertools.product(range(1, chips), range(PARTS)):
        forward(near, h, False)
    for c, h, j in itertools.product(range(chips), range(PARTS), range(per_section)):
        d = c * CORES + 1 - core
        place = kv_place(j, d, h)
        pltpu.make_async_copy(place, place, kv_recv.at[j, d, h]).wait()
        keep(j, d, h, chips + c).start()
    send_kv(True)
    send_q(range(ranks), True)
    for h in range(PARTS):
        if not stay:
            relay(h, True)
        for near in range(chips):
            forward(near, h, True)
    for c, h, j in itertools.product(range(chips), range(PARTS), range(per_section)):
        keep(j, c * CORES + 1 - core, h, chips + c).wait()
    for j in range(per_section):
        for d in range(ranks):
            pltpu.make_async_copy(q_place(j, d), q_place(j, d), q_recv.at[j, d]).wait()


def route(folded_q, folded_kv, table, number):
    per_section, ranks, rows, _ = folded_q.shape
    key_heads = folded_kv.shape[1]
    chips = ranks // CORES
    dma = pltpu.SemaphoreType.DMA
    return pl.pallas_call(
        functools.partial(route_kernel, table, per_section),
        out_shape=jax.ShapeDtypeStruct(
            (per_section, 1, ranks * rows, 3 * FACE_SPAN), jnp.bfloat16
        ),
        in_specs=[pl.BlockSpec(memory_space=pl.ANY)] * 2,
        out_specs=pl.BlockSpec(memory_space=pl.ANY),
        scratch_shapes=[
            dma((per_section, ranks)),
            dma((per_section, ranks)),
            dma((per_section, key_heads, PARTS)),
            dma((per_section, ranks, PARTS)),
            dma((per_section, chips, PARTS)),
            dma((per_section, chips, PARTS, 2)),
            pltpu.VMEM((per_section, ranks, rows, 2 * FACE_SPAN), jnp.bfloat16),
            dma((per_section, ranks, PARTS)),
            pltpu.VMEM((per_section, key_heads, rows, 2 * FACE_SPAN), jnp.bfloat16),
            dma((per_section, key_heads, PARTS)),
            dma((per_section, key_heads, PARTS)),
        ],
        compiler_params=pltpu.CompilerParams(collective_id=number, has_side_effects=True),
        name="route",
    )(folded_q, folded_kv)


def direct(
    wq_train, lock_learned_mats, worth_learned_mats, gain_train, train_slots, serve_section, face_sequence
):
    sections = lax.axis_size("pa")
    per_section = wq_train.shape[0]
    groups = sections // per_section
    my = lax.axis_index("pa").astype(jnp.int32).reshape(1)
    folded_q, folded_kv = fold(
        wq_train, lock_learned_mats, worth_learned_mats, gain_train,
        my, train_slots, serve_section, face_sequence, sections,
    )
    routes = routes_of(sections, per_section)
    weights = groups ** jnp.arange(sections, dtype=jnp.int32)
    code = jnp.sum(serve_section % groups * weights)
    chosen = jnp.int32(0)
    for i, table in enumerate(routes):
        known = sum(own * groups**q for q, own in enumerate(table))
        chosen = jnp.where(code == known, i, chosen)
    return lax.switch(
        chosen,
        [functools.partial(route, table=t, number=i) for i, t in enumerate(routes)],
        folded_q,
        folded_kv,
    )


def fits(sections, per_section, ranks, query_heads, key_heads):
    if sections % per_section or ranks % (CORES * key_heads) or query_heads != ranks:
        return False
    ways, left = 1, sections
    while left:
        ways, left = ways * math.comb(left, per_section), left - per_section
    return ways <= MAX_ROUTES


def move(*arrays):
    wq_train, lock_learned_mats = arrays[:2]
    plain = fits(
        lax.axis_size("pa"),
        wq_train.shape[0],
        lax.axis_size("dev"),
        wq_train.shape[2] // FACE_SPAN,
        lock_learned_mats.shape[2] // FACE_SPAN,
    )
    return direct(*arrays) if plain else local(*arrays)


def solution(mesh):
    return jax.shard_map(
        move,
        mesh=mesh,
        in_specs=(
            P("pa", "dev", None),
            P("pa", "dev", None),
            P("pa", "dev", None),
            P("pa", "dev"),
            P(),
            P(),
            P(),
        ),
        out_specs=P("pa", "dev", None, None),
        check_vma=False,
    )
```

```python
import functools
import itertools
import math

import jax
import jax.numpy as jnp
from jax import lax
from jax.experimental import pallas as pl
from jax.experimental.pallas import tpu as pltpu
from jax.sharding import PartitionSpec as P

FACE_SPAN = 128
GROUP = 4


def lookup(small_table, indices):
    entries = jnp.arange(small_table.shape[0], dtype=jnp.int32)
    return jnp.sum(jnp.where(indices[..., None] == entries, small_table, 0), axis=-1).astype(
        jnp.int32
    )


def local(
    wq_train,
    lock_learned_mats,
    worth_learned_mats,
    gain_train,
    train_slots,
    serve_section,
    face_sequence,
):
    per_section = wq_train.shape[0]
    row_count = wq_train.shape[1]
    query_width = wq_train.shape[2]
    key_width = lock_learned_mats.shape[2]
    query_heads = query_width // FACE_SPAN
    key_heads = key_width // FACE_SPAN
    sections = lax.axis_size("pa")
    rank_count = lax.axis_size("dev")
    my_section = lax.axis_index("pa")
    keys_each = max(key_heads // rank_count, 1)
    slot_ids = jnp.arange(train_slots.shape[0], dtype=jnp.int32)
    section_ids = jnp.arange(sections, dtype=jnp.int32)
    slot_index = jnp.arange(per_section, dtype=jnp.int32)
    folded = (
        jnp.concatenate([wq_train, lock_learned_mats, worth_learned_mats], axis=2)
        * gain_train[:, :, None]
    )
    folded = folded.astype(jnp.bfloat16)

    def source_slot(layers):
        return jnp.sum(jnp.where(train_slots == layers[..., None], slot_ids, 0), axis=-1).astype(
            jnp.int32
        )

    wanted_layers = lookup(serve_section, my_section) * per_section + slot_index
    held_layers = lookup(train_slots, my_section * per_section + slot_index)
    destination = jnp.sum(
        jnp.where(
            serve_section[None, :] == (held_layers // per_section)[:, None], section_ids[None, :], 0
        ),
        axis=-1,
    )
    send_pick = (destination[None, :] == section_ids[:, None]).astype(jnp.bfloat16)
    outgoing = jnp.einsum(
        "qj,jrc->qrc", send_pick, folded, preferred_element_type=jnp.float32
    ).astype(jnp.bfloat16)
    arrived = lax.all_to_all(outgoing, "pa", split_axis=0, concat_axis=0, tiled=True)
    anchor = source_slot(wanted_layers) // per_section
    recv_pick = (anchor[:, None] == section_ids[None, :]).astype(jnp.bfloat16)
    received = jnp.einsum(
        "jq,qrc->jrc", recv_pick, arrived, preferred_element_type=jnp.float32
    ).astype(jnp.bfloat16)
    head_index = jnp.arange(query_heads, dtype=jnp.int32)
    pair_number = (
        jnp.arange(rank_count, dtype=jnp.int32)[:, None] * key_heads // rank_count
        + jnp.arange(keys_each, dtype=jnp.int32)[None, :]
    )

    def arrange(layer_rows, layer_id):
        group_order = jnp.take(face_sequence, layer_id, axis=0)
        q_source = lookup(group_order, head_index // GROUP) * GROUP + head_index % GROUP
        pair_provider = lookup(group_order, pair_number).reshape(-1)
        query_part = layer_rows[:, :query_width].reshape(row_count, query_heads, FACE_SPAN)
        key_part = layer_rows[:, query_width : query_width + key_width].reshape(
            row_count, key_heads, FACE_SPAN
        )
        value_part = layer_rows[:, query_width + key_width :].reshape(
            row_count, key_heads, FACE_SPAN
        )
        query_sel = jnp.take(query_part, q_source, axis=1).reshape(
            row_count, rank_count, query_heads // rank_count, FACE_SPAN
        )
        lock_picker = jnp.take(key_part, pair_provider, axis=1).reshape(
            row_count, rank_count, keys_each, FACE_SPAN
        )
        worth_picker = jnp.take(value_part, pair_provider, axis=1).reshape(
            row_count, rank_count, keys_each, FACE_SPAN
        )
        joined_cols = jnp.concatenate([query_sel, lock_picker, worth_picker], axis=2)
        return joined_cols.transpose(1, 0, 2, 3).reshape(rank_count, row_count, -1)

    collected = []
    for slot in range(per_section):
        outgoing_cols = arrange(received[slot], wanted_layers[slot])
        collected.append(
            lax.all_to_all(outgoing_cols, "dev", split_axis=0, concat_axis=1, tiled=True)
        )
    result = jnp.stack(collected, axis=0)
    return result

MESH = pl.DeviceIdType.MESH
CORES = 2
MAX_ROUTES = 8
PARTS = 4


def routes_of(sections, per_section):
    groups = sections // per_section
    base = [g for g in range(groups) for _ in range(per_section)]
    seen = []
    for choice in itertools.product(range(groups), repeat=sections):
        if sorted(choice) == base:
            seen.append(choice)
    return seen


def section_route(table, section, ordinal, per_section):
    dest = 0
    for g in range(max(table) + 1):
        members = [q for q, own in enumerate(table) if own == g]
        dest = jnp.where(section // per_section == g, members[ordinal], dest)
    return dest


def fold_kernel(
    sizes, my_ref, slots_ref, serve_ref, face_ref, wq_ref, lock_ref, worth_ref, gain_ref, q_out, kv_out
):
    sections, per_section, query_heads, key_heads = sizes
    layer, slot = pick(sizes, pl.program_id(0), my_ref, slots_ref, serve_ref)
    row = gain_ref[0:1]
    for i in range(1, per_section):
        row = jnp.where(slot == i, gain_ref[i : i + 1], row)
    gain = jnp.broadcast_to(row, (FACE_SPAN, row.shape[1])).T
    for h in range(query_heads):
        source = face_ref[h // GROUP, layer] * GROUP + h % GROUP
        cols = pl.ds(pl.multiple_of(source * FACE_SPAN, FACE_SPAN), FACE_SPAN)
        q_out[0, h] = (wq_ref[0, :, cols] * gain).astype(jnp.bfloat16)
    for g in range(key_heads):
        cols = pl.ds(pl.multiple_of(face_ref[g, layer] * FACE_SPAN, FACE_SPAN), FACE_SPAN)
        kv_out[0, g, :, :FACE_SPAN] = (lock_ref[0, :, cols] * gain).astype(jnp.bfloat16)
        kv_out[0, g, :, FACE_SPAN:] = (worth_ref[0, :, cols] * gain).astype(jnp.bfloat16)


def pick(sizes, ordinal, my_ref, slots_ref, serve_ref):
    sections, per_section, _, _ = sizes
    groups = sections // per_section
    mine = my_ref[0]
    block, count = jnp.int32(0), jnp.int32(0)
    for q in range(sections):
        own = serve_ref[q] % groups == mine // per_section
        block = jnp.where(own & (count == ordinal), serve_ref[q], block)
        count = count + own.astype(jnp.int32)
    layer = block * per_section + mine % per_section
    slot = jnp.int32(0)
    for i in range(per_section):
        slot = jnp.where(slots_ref[mine * per_section + i] == layer, i, slot)
    return layer, slot


def fold(wq, lock, worth, gain, my, slots, serve, face, sections):
    per_section, rows, query_width = wq.shape
    key_width = lock.shape[2]
    query_heads, key_heads = query_width // FACE_SPAN, key_width // FACE_SPAN
    sizes = (sections, per_section, query_heads, key_heads)
    tile = min(rows, 256)

    def source(o, i, my_ref, slots_ref, serve_ref, face_ref):
        return (pick(sizes, o, my_ref, slots_ref, serve_ref)[1], i, 0)

    def target(o, i, *_):
        return (o, 0, i, 0)

    return pl.pallas_call(
        functools.partial(fold_kernel, sizes),
        grid_spec=pltpu.PrefetchScalarGridSpec(
            num_scalar_prefetch=4,
            grid=(per_section, rows // tile),
            in_specs=[
                pl.BlockSpec((1, tile, query_width), source),
                pl.BlockSpec((1, tile, key_width), source),
                pl.BlockSpec((1, tile, key_width), source),
                pl.BlockSpec((per_section, tile), lambda o, i, *_: (0, i)),
            ],
            out_specs=[
                pl.BlockSpec((1, query_heads, tile, FACE_SPAN), target),
                pl.BlockSpec((1, key_heads, tile, 2 * FACE_SPAN), target),
            ],
        ),
        out_shape=[
            jax.ShapeDtypeStruct((per_section, query_heads, rows, FACE_SPAN), jnp.bfloat16),
            jax.ShapeDtypeStruct((per_section, key_heads, rows, 2 * FACE_SPAN), jnp.bfloat16),
        ],
        name="fold",
    )(my, slots, serve, face.T, wq, lock, worth, gain)


def route_kernel(
    table, per_section, q_ref, kv_ref, out_ref, q_send, q_recv, kv_send, kv_recv, near_send, far_send, kv_held, kept,
    passing, pass_send, pass_recv
):
    sections = len(table)
    ranks = q_ref.shape[1]
    key_heads = kv_ref.shape[1]
    rows = q_ref.shape[2]
    chips = ranks // CORES
    span = chips // key_heads
    section = lax.axis_index("pa")
    rank = lax.axis_index("dev")
    chip, core = rank // CORES, rank % CORES
    slot = section % per_section
    stay = all(own == q // per_section for q, own in enumerate(table))

    barrier = pltpu.get_barrier_semaphore()

    def greet(i, carry):
        other = (section * ranks + rank + i) % (sections * ranks)
        pl.semaphore_signal(
            barrier, inc=1, device_id=(other // ranks, other % ranks), device_id_type=MESH
        )
        return carry

    lax.fori_loop(1, sections * ranks, greet, 0)
    pl.semaphore_wait(barrier, sections * ranks - 1)

    def q_place(j, d):
        return out_ref.at[j, 0, pl.ds(pl.multiple_of(d * rows, rows), rows), pl.ds(0, FACE_SPAN)]

    part = rows // PARTS

    def kv_place(j, d, h):
        return kv_held.at[j, d, pl.ds(h * part, part)]

    def keep(j, d, h, index):
        first = pl.multiple_of(d * rows + h * part, part)
        place = out_ref.at[j, 0, pl.ds(first, part), pl.ds(FACE_SPAN, 2 * FACE_SPAN)]
        return pltpu.make_async_copy(kv_place(j, d, h), place, kept.at[j, index, h])

    def send(source, place, send_sem, recv_sem, to, wait=False):
        here = (to[0] == section) & (to[1] == rank)

        @pl.when(jnp.logical_not(here))
        def _():
            copy = pltpu.make_async_remote_copy(
                source, place, send_sem, recv_sem, device_id=to, device_id_type=MESH
            )
            copy.wait_send() if wait else copy.start()

        if not wait:

            @pl.when(here)
            def _():
                pltpu.make_async_copy(source, place, recv_sem).start()

    def send_kv(wait):
        for h, g, o in itertools.product(range(PARTS), range(key_heads), range(per_section)):
            to = section_route(table, section, o, per_section)
            source = kv_ref.at[o, g, pl.ds(h * part, part)]
            sent = kv_send.at[o, g, h]
            if stay:
                entry = jnp.clip(chip, g * span, g * span + span - 1)
                send(
                    source, kv_place(slot, rank, h), sent, kv_recv.at[slot, rank, h],
                    (to, entry * CORES + core), wait,
                )
                continue

            @pl.when(chip // span == g)
            def _():
                send(
                    source, kv_place(slot, rank, h), sent, kv_recv.at[slot, rank, h],
                    (to, rank), wait,
                )

            @pl.when(chip // span != g)
            def _():
                send(
                    source, pass_place(slot, g, h), sent, pass_recv.at[slot, g, h],
                    (to, rank), wait,
                )

    def pass_place(j, g, h):
        return passing.at[j, g, pl.ds(h * part, part)]

    def relay(h, wait):
        for g, j in itertools.product(range(key_heads), range(per_section)):

            @pl.when(chip // span != g)
            def _():
                place = pass_place(j, g, h)
                entry = jnp.clip(chip, g * span, g * span + span - 1)
                if not wait:
                    pltpu.make_async_copy(place, place, pass_recv.at[j, g, h]).wait()
                copy = pltpu.make_async_remote_copy(
                    place, kv_place(j, rank, h), pass_send.at[j, g, h], kv_recv.at[j, rank, h],
                    device_id=(section, entry * CORES + core),
                    device_id_type=MESH,
                )
                copy.wait_send() if wait else copy.start()

    def send_q(steps, wait):
        for step in steps:
            for o in range(per_section):
                to = section_route(table, section, o, per_section)
                r = (rank + ranks // 2 + step) % ranks
                send(
                    q_ref.at[o, r], q_place(slot, rank), q_send.at[o, step], q_recv.at[slot, rank],
                    (to, r), wait,
                )

    def forward(near, h, wait):
        low = chip // span * span
        high = low + span - 1
        turn = jnp.where(chip < chips // 2, 1, chips - 1)
        for j in range(per_section):
            c = (chip + turn * near) % chips
            d = c * CORES + core
            place = kv_place(j, d, h)
            entry = jnp.clip(c, low, high)
            if not wait:
                pltpu.make_async_copy(place, place, kv_recv.at[j, d, h]).wait()
            for up in (1, 0):
                go = (
                    (chip >= entry) & (chip < high) if up else (chip <= entry) & (chip > low)
                )

                @pl.when(go)
                def _():
                    copy = pltpu.make_async_remote_copy(
                        place, place, far_send.at[j, near, h, up], kv_recv.at[j, d, h],
                        device_id=(section, (chip + 2 * up - 1) * CORES + core),
                        device_id_type=MESH,
                    )
                    copy.wait_send() if wait else copy.start()

            copy = pltpu.make_async_remote_copy(
                place, place, near_send.at[j, near, h], kv_recv.at[j, d, h],
                device_id=(section, chip * CORES + 1 - core),
                device_id_type=MESH,
            )
            copy.wait_send() if wait else copy.start()
            copy = keep(j, d, h, near)
            copy.wait() if wait else copy.start()

    send_kv(False)
    if stay:
        send_q(range(ranks), False)
    for h in range(PARTS):
        if not stay:
            send_q(range(ranks * h // PARTS, ranks * (h + 1) // PARTS), False)
            relay(h, False)
        forward(0, h, False)
    for near, h in itertools.product(range(1, chips), range(PARTS)):
        forward(near, h, False)
    for c, h, j in itertools.product(range(chips), range(PARTS), range(per_section)):
        d = c * CORES + 1 - core
        place = kv_place(j, d, h)
        pltpu.make_async_copy(place, place, kv_recv.at[j, d, h]).wait()
        keep(j, d, h, chips + c).start()
    send_kv(True)
    send_q(range(ranks), True)
    for h in range(PARTS):
        if not stay:
            relay(h, True)
        for near in range(chips):
            forward(near, h, True)
    for c, h, j in itertools.product(range(chips), range(PARTS), range(per_section)):
        keep(j, c * CORES + 1 - core, h, chips + c).wait()
    for j in range(per_section):
        for d in range(ranks):
            pltpu.make_async_copy(q_place(j, d), q_place(j, d), q_recv.at[j, d]).wait()


def route(folded_q, folded_kv, table, number):
    per_section, ranks, rows, _ = folded_q.shape
    key_heads = folded_kv.shape[1]
    chips = ranks // CORES
    dma = pltpu.SemaphoreType.DMA
    return pl.pallas_call(
        functools.partial(route_kernel, table, per_section),
        out_shape=jax.ShapeDtypeStruct(
            (per_section, 1, ranks * rows, 3 * FACE_SPAN), jnp.bfloat16
        ),
        in_specs=[pl.BlockSpec(memory_space=pl.ANY)] * 2,
        out_specs=pl.BlockSpec(memory_space=pl.ANY),
        scratch_shapes=[
            dma((per_section, ranks)),
            dma((per_section, ranks)),
            dma((per_section, key_heads, PARTS)),
            dma((per_section, ranks, PARTS)),
            dma((per_section, chips, PARTS)),
            dma((per_section, chips, PARTS, 2)),
            pltpu.VMEM((per_section, ranks, rows, 2 * FACE_SPAN), jnp.bfloat16),
            dma((per_section, ranks, PARTS)),
            pltpu.VMEM((per_section, key_heads, rows, 2 * FACE_SPAN), jnp.bfloat16),
            dma((per_section, key_heads, PARTS)),
            dma((per_section, key_heads, PARTS)),
        ],
        compiler_params=pltpu.CompilerParams(collective_id=number, has_side_effects=True),
        name="route",
    )(folded_q, folded_kv)


def direct(
    wq_train, lock_learned_mats, worth_learned_mats, gain_train, train_slots, serve_section, face_sequence
):
    sections = lax.axis_size("pa")
    per_section = wq_train.shape[0]
    groups = sections // per_section
    my = lax.axis_index("pa").astype(jnp.int32).reshape(1)
    folded_q, folded_kv = fold(
        wq_train, lock_learned_mats, worth_learned_mats, gain_train,
        my, train_slots, serve_section, face_sequence, sections,
    )
    routes = routes_of(sections, per_section)
    weights = groups ** jnp.arange(sections, dtype=jnp.int32)
    code = jnp.sum(serve_section % groups * weights)
    chosen = jnp.int32(0)
    for i, table in enumerate(routes):
        known = sum(own * groups**q for q, own in enumerate(table))
        chosen = jnp.where(code == known, i, chosen)
    return lax.switch(
        chosen,
        [functools.partial(route, table=t, number=i) for i, t in enumerate(routes)],
        folded_q,
        folded_kv,
    )


def fits(sections, per_section, ranks, query_heads, key_heads):
    if sections % per_section or ranks % (CORES * key_heads) or query_heads != ranks:
        return False
    ways, left = 1, sections
    while left:
        ways, left = ways * math.comb(left, per_section), left - per_section
    return ways <= MAX_ROUTES


def move(*arrays):
    wq_train, lock_learned_mats = arrays[:2]
    plain = fits(
        lax.axis_size("pa"),
        wq_train.shape[0],
        lax.axis_size("dev"),
        wq_train.shape[2] // FACE_SPAN,
        lock_learned_mats.shape[2] // FACE_SPAN,
    )
    return direct(*arrays) if plain else local(*arrays)


def solution(mesh):
    return jax.shard_map(
        move,
        mesh=mesh,
        in_specs=(
            P("pa", "dev", None),
            P("pa", "dev", None),
            P("pa", "dev", None),
            P("pa", "dev"),
            P(),
            P(),
            P(),
        ),
        out_specs=P("pa", "dev", None, None),
        check_vma=False,
    )
```
